32 devices in a mesh: dev: 32 (over z, y, x, core).
Axes of the slice: x: 2, y: 2, z: 4, core: 2. Of those that a mesh axis runs over, the one named last changes fastest.
Arguments:
- tokens: bfloat16 [24576, 1088], P('dev'), may hold values from -6 to 6
- cotangent: bfloat16 [24576, 1088], P('dev'), may hold values from -6 to 6
- segments: int32 [24576], P('dev'), may hold values from -1 to 5, as said below
- attention_flat: bfloat16 [36992, 128], P('dev')
- feedforward_flat: bfloat16 [73984, 128], P('dev')
- vectors: bfloat16 [13056], P('dev')
Outputs:
- layer_output: bfloat16 [24576, 1088], P('dev')
- token_gradient: float32 [24576, 1088], P('dev')
- attention_gradient: float32 [36992, 128], P('dev')
- feedforward_gradient: float32 [73984, 128], P('dev')
- vector_gradient: float32 [13056], P('dev')
The draws below stay inside these ranges and needn't reach their ends.
Inputs may be any that keep to these rules, and one draw needn't show every extreme that they name: `segments`: in each slab of 768 slots the first 128 k slots are live (1 <= k <= 6) and the rest are -1. Live slots carry sequence numbers 0, 1, 2, ... that never fall from one slot to the next and start at 0; a slab holds at most 6 sequences. In every draw some slab is fully live and holds exactly 6 sequences, and some slab has padding.
All inputs are finite; a program needn't handle non-finite values.
Results may differ from the reference program's by a relative error of at most 0.013.
The reference program's roundings to bfloat16 on the way count: a program that leaves them out, or rounds other values in their place, can miss the bound.
Values may be sent and summed in bfloat16 or wider, within the bound.
A program may use at most 320 MiB of HBM per device.

```python
import jax
import jax.numpy as jnp
from jax import lax

D = 1088
HEAD_DIM = 64
FF = 4352
BLOCK = 128
LANES = 128
TOK_DEV = 768
TOKENS = 24576
N_DEV = 32


start_odds = 320


def draw_segments(key, part):
    slab_count = TOKENS // TOK_DEV
    block_count = TOK_DEV // BLOCK
    key_list = jax.random.split(jax.random.fold_in(key, 11), 4)
    live_blocks = jax.random.randint(key_list[0], (slab_count,), 1, block_count + 1)
    full_slab = jax.random.randint(key_list[1], (), 0, slab_count)
    short_slab = (full_slab + 1 + jax.random.randint(key_list[2], (), 0, slab_count - 1)) % slab_count
    live_blocks = live_blocks.at[full_slab].set(block_count)
    live_blocks = live_blocks.at[short_slab].set(jnp.minimum(live_blocks[short_slab], block_count - 1))
    starts = jax.random.randint(key_list[3], (slab_count, TOK_DEV), 0, start_odds) == 0
    positions = lax.broadcasted_iota(jnp.int32, (slab_count, TOK_DEV), 1)
    slab_numbers = lax.broadcasted_iota(jnp.int32, (slab_count, TOK_DEV), 0)
    forced = (slab_numbers == full_slab) & (positions % BLOCK == 0)
    starts = jnp.logical_or(jnp.logical_or(starts, positions == 0), forced)
    numbers = jnp.minimum(jnp.cumsum(starts.astype(jnp.int32), axis=1) - 1, block_count - 1)
    live_mask = positions < (live_blocks * BLOCK)[:, None]
    return jnp.where(live_mask, numbers, -1).reshape(-1).astype(jnp.int32)


def draw_attention_flat(key, part):
    row_total = 4 * D * D // LANES
    shape_pair = (row_total, LANES)
    flat_index = lax.broadcasted_iota(jnp.int32, shape_pair, 0) * LANES + lax.broadcasted_iota(jnp.int32, shape_pair, 1)
    column = flat_index % (3 * D)
    joint_part = flat_index < 3 * D * D
    base = jax.random.normal(key, shape_pair, jnp.float32)
    joint_scale = jnp.where(column < 2 * D, 1.0, 1.0)
    scale_rows = jnp.where(joint_part, joint_scale * D ** (-0.5), 4.0 * D ** (-0.5))
    return (base * scale_rows).astype(jnp.bfloat16)


def draw_feedforward_flat(key, part):
    row_total = 2 * D * FF // LANES
    shape_pair = (row_total, LANES)
    flat_index = lax.broadcasted_iota(jnp.int32, shape_pair, 0) * LANES + lax.broadcasted_iota(jnp.int32, shape_pair, 1)
    base = jax.random.normal(key, shape_pair, jnp.float32)
    scale_rows = jnp.where(flat_index < D * FF, D ** (-0.5), FF ** (-0.5))
    return (base * scale_rows).astype(jnp.bfloat16)


def draw_vectors(key, part):
    entry_count = 8 * D + FF
    base = jax.random.normal(key, (entry_count,), jnp.float32)
    which_slot = jnp.arange(entry_count, dtype=jnp.int32) // D
    is_gain = (which_slot == 0) | (which_slot == 5)
    return jnp.where(is_gain, 1.0 + 0.2 * base, 0.5 * base).astype(jnp.bfloat16)


def steps_of(stream_key, extent, pieces, low, high):
    loudness, own = 1.0, jax.random.fold_in(stream_key, 6)
    for dim, blocks in pieces:
        heights = jnp.exp(jax.random.uniform(jax.random.fold_in(own, dim), (blocks,), jnp.float32, low / len(pieces), high / len(pieces)))
        loudness = loudness * jnp.repeat(heights, extent[dim] // blocks).reshape([-1 if axis == dim else 1 for axis in range(len(extent))])
    return loudness


def centred(stream_key, extent, width, bound, cuts=(), kind=jnp.bfloat16):
    values = jax.random.normal(stream_key, extent, jnp.float32) * width
    if len(cuts) > 0:
        values = steps_of(stream_key, extent, cuts, -0.22, 0.18) * values
    return jnp.clip(values, min=-bound, max=bound).astype(kind)


def setup_inputs(seed: int = 0) -> dict:
    splits = jax.random.split(jax.random.key(seed), 7)
    tokens = centred(splits[0], (TOKENS, D), 1.0, 6.0, ((0, 32),))
    cotangent = centred(splits[1], (TOKENS, D), 1.0, 6.0, ((0, 32),))
    segments = draw_segments(jax.random.fold_in(splits[6], 71), 0)
    attention_flat = draw_attention_flat(jax.random.fold_in(splits[6], 71), 0)
    feedforward_flat = draw_feedforward_flat(jax.random.fold_in(splits[6], 71), 0)
    vectors = draw_vectors(jax.random.fold_in(splits[6], 71), 0)
    return dict(tokens=tokens, cotangent=cotangent, segments=segments, attention_flat=attention_flat, feedforward_flat=feedforward_flat, vectors=vectors)


norm_epsilon = 1e-05
masked_score = -1e+30

def gaussian_unit(values):
    return jax.nn.gelu(values, approximate=True)

def rounded(values):
    return lax.optimization_barrier(values.astype(jnp.bfloat16))

def normalize(matrix):
    center = lax.optimization_barrier(jnp.mean(matrix, axis=-1, keepdims=True))
    deviation = matrix - center
    variance = lax.optimization_barrier(jnp.mean(deviation * deviation, axis=-1, keepdims=True))
    inverse = lax.rsqrt(variance + norm_epsilon)
    return (deviation * inverse, inverse)

def normalize_back(normed_grad, normed, inverse):
    first_mean = lax.optimization_barrier(jnp.mean(normed_grad, axis=-1, keepdims=True))
    second_mean = lax.optimization_barrier(jnp.mean(normed_grad * normed, axis=-1, keepdims=True))
    return inverse * (normed_grad - first_mean - normed * second_mean)

def open_attention(flat_rows, features):
    flattened = flat_rows.reshape(-1)
    boundary = 3 * features * features
    return (flattened[:boundary].reshape(features, 3 * features), flattened[boundary:].reshape(features, features))

def open_feedforward(flat_rows, features):
    flattened = flat_rows.reshape(-1)
    hidden_units = flattened.shape[0] // (2 * features)
    boundary = features * hidden_units
    return (flattened[:boundary].reshape(features, hidden_units), flattened[boundary:].reshape(hidden_units, features))

def open_vectors(vector_rows, features):
    widened = vector_rows.astype(jnp.float32)
    return (widened[:8 * features].reshape(8, features), widened[8 * features:])

def slab_pass(tokens, cotangent, segments, joint_weight, output_weight, expand_weight, contract_weight, gains_biases, expand_bias):
    row_count, features = tokens.shape
    head_count = features // HEAD_DIM
    head_shape = (row_count, head_count, HEAD_DIM)
    score_scale = HEAD_DIM ** (-0.5)
    live_rows = (segments >= 0)[:, None]
    positions = jnp.arange(row_count, dtype=jnp.int32)
    visible = (segments[:, None] == segments[None, :]) & (positions[None, :] <= positions[:, None])
    inputs = tokens.astype(jnp.float32)
    normed_one, inverse_one = normalize(inputs)
    attention_input = (normed_one * gains_biases[0] + gains_biases[1]).astype(jnp.bfloat16)
    joint_out = jnp.dot(attention_input, joint_weight, preferred_element_type=jnp.float32)
    queries = rounded(joint_out[:, :features] + gains_biases[2])
    keys_low = rounded(joint_out[:, features:2 * features])
    values_low = rounded(joint_out[:, 2 * features:] + gains_biases[3])
    query_heads = queries.astype(jnp.float32).reshape(head_shape)
    key_heads = keys_low.astype(jnp.float32).reshape(head_shape)
    value_heads = values_low.astype(jnp.float32).reshape(head_shape)
    scores = score_scale * jnp.einsum('qhd,khd->hqk', query_heads, key_heads)
    scores = jnp.where(visible[None], scores, masked_score)
    highest = lax.optimization_barrier(jnp.max(scores, axis=-1, keepdims=True))
    log_total = highest + jnp.log(lax.optimization_barrier(jnp.sum(jnp.exp(scores - highest), axis=-1, keepdims=True)))
    weights = jnp.exp(scores - log_total)
    prob_values = rounded(weights).astype(jnp.float32)
    mixed_rows = rounded(jnp.einsum('hqk,khd->qhd', prob_values, value_heads).reshape(row_count, features))
    residual = inputs + jnp.dot(mixed_rows, output_weight, preferred_element_type=jnp.float32) + gains_biases[4]
    normed_two, inverse_two = normalize(residual)
    feedforward_input = (normed_two * gains_biases[5] + gains_biases[6]).astype(jnp.bfloat16)
    pre_activation = jnp.dot(feedforward_input, expand_weight, preferred_element_type=jnp.float32) + expand_bias
    activation = gaussian_unit(pre_activation).astype(jnp.bfloat16)
    final_rows = residual + jnp.dot(activation, contract_weight, preferred_element_type=jnp.float32) + gains_biases[7]
    layer_output = jnp.where(live_rows, final_rows, 0.0).astype(jnp.bfloat16)
    upstream = jnp.where(live_rows, cotangent.astype(jnp.float32), 0.0)
    upstream_low = upstream.astype(jnp.bfloat16)
    contract_grad = jnp.dot(activation.T, upstream_low, preferred_element_type=jnp.float32)
    contract_bias_grad = lax.optimization_barrier(jnp.sum(upstream, axis=0))
    activation_grad = jnp.dot(upstream_low, contract_weight.T, preferred_element_type=jnp.float32)
    unused_value, gelu_pullback = jax.vjp(gaussian_unit, pre_activation)
    pre_grad = gelu_pullback(activation_grad)[0]
    pre_grad_low = pre_grad.astype(jnp.bfloat16)
    expand_grad = jnp.dot(feedforward_input.T, pre_grad_low, preferred_element_type=jnp.float32)
    expand_bias_grad = lax.optimization_barrier(jnp.sum(pre_grad, axis=0))
    second_grad = jnp.dot(pre_grad_low, expand_weight.T, preferred_element_type=jnp.float32)
    second_gain_grad = lax.optimization_barrier(jnp.sum(second_grad * normed_two, axis=0))
    second_bias_grad = lax.optimization_barrier(jnp.sum(second_grad, axis=0))
    residual_grad = upstream + normalize_back(second_grad * gains_biases[5], normed_two, inverse_two)
    residual_low = residual_grad.astype(jnp.bfloat16)
    output_grad = jnp.dot(mixed_rows.T, residual_low, preferred_element_type=jnp.float32)
    output_bias_grad = lax.optimization_barrier(jnp.sum(residual_grad, axis=0))
    mixed_grad = rounded(jnp.dot(residual_low, output_weight.T, preferred_element_type=jnp.float32))
    mixed_grad_heads = mixed_grad.astype(jnp.float32).reshape(head_shape)
    mixed_heads = mixed_rows.astype(jnp.float32).reshape(head_shape)
    prob_grad = jnp.einsum('qhd,khd->hqk', mixed_grad_heads, value_heads)
    row_delta = jnp.einsum('qhd,qhd->hq', mixed_grad_heads, mixed_heads)
    score_grad = rounded(score_scale * weights * (prob_grad - row_delta[:, :, None])).astype(jnp.float32)
    query_grad = jnp.einsum('hqk,khd->qhd', score_grad, key_heads).reshape(row_count, features)
    key_grad = jnp.einsum('hqk,qhd->khd', score_grad, query_heads).reshape(row_count, features)
    value_grad = jnp.einsum('hqk,qhd->khd', prob_values, mixed_grad_heads).reshape(row_count, features)
    joint_grad = jnp.concatenate([query_grad, key_grad, value_grad], axis=1)
    joint_low = joint_grad.astype(jnp.bfloat16)
    joint_weight_grad = jnp.dot(attention_input.T, joint_low, preferred_element_type=jnp.float32)
    first_grad = jnp.dot(joint_low, joint_weight.T, preferred_element_type=jnp.float32)
    first_gain_grad = lax.optimization_barrier(jnp.sum(first_grad * normed_one, axis=0))
    first_bias_grad = lax.optimization_barrier(jnp.sum(first_grad, axis=0))
    token_gradient = residual_grad + normalize_back(first_grad * gains_biases[0], normed_one, inverse_one)
    vector_grad = jnp.concatenate([first_gain_grad, first_bias_grad, lax.optimization_barrier(jnp.sum(query_grad, axis=0)), lax.optimization_barrier(jnp.sum(value_grad, axis=0)), output_bias_grad, second_gain_grad, second_bias_grad, contract_bias_grad, expand_bias_grad])
    return (layer_output, token_gradient, (joint_weight_grad, output_grad, expand_grad, contract_grad, vector_grad))

def reference(tokens, cotangent, segments, attention_flat, feedforward_flat, vectors):
    features = tokens.shape[1]
    joint_weight, output_weight = open_attention(attention_flat, features)
    expand_weight, contract_weight = open_feedforward(feedforward_flat, features)
    gains_biases, expand_bias = open_vectors(vectors, features)
    slab_tokens = tokens.reshape(N_DEV, -1, features)
    slab_cotangent = cotangent.reshape(N_DEV, -1, features)
    slab_segments = segments.reshape(N_DEV, -1)

    def visit(running, slab_item):
        layer_output, token_gradient, slab_grads = slab_pass(slab_item[0], slab_item[1], slab_item[2], joint_weight, output_weight, expand_weight, contract_weight, gains_biases, expand_bias)
        return (jax.tree.map(jnp.add, running, slab_grads), (layer_output, token_gradient))
    zero_grads = (jnp.zeros(joint_weight.shape, jnp.float32), jnp.zeros(output_weight.shape, jnp.float32), jnp.zeros(expand_weight.shape, jnp.float32), jnp.zeros(contract_weight.shape, jnp.float32), jnp.zeros(vectors.shape, jnp.float32))
    running, outputs = lax.scan(visit, zero_grads, (slab_tokens, slab_cotangent, slab_segments))
    attention_gradient = jnp.concatenate([running[0].reshape(-1), running[1].reshape(-1)]).reshape(-1, LANES)
    feedforward_gradient = jnp.concatenate([running[2].reshape(-1), running[3].reshape(-1)]).reshape(-1, LANES)
    return (outputs[0].reshape(-1, features), outputs[1].reshape(-1, features), attention_gradient, feedforward_gradient, running[4])
```

```python
import functools

import jax
import jax.numpy as jnp
from jax import lax
from jax.experimental import pallas as pl
from jax.experimental.pallas import tpu as pltpu
from jax.sharding import PartitionSpec as P

HEAD_DIM = 64
LANES = 128

norm_epsilon = 1e-05
masked_score = -1e30


def gaussian_unit(values):
    return jax.nn.gelu(values, approximate=True)


def normalize(matrix):
    center = jnp.mean(matrix, axis=-1, keepdims=True)
    deviation = matrix - center
    variance = jnp.mean(deviation * deviation, axis=-1, keepdims=True)
    inverse = lax.rsqrt(variance + norm_epsilon)
    return (deviation * inverse, inverse)


def normalize_back(normed_grad, normed, inverse):
    first_mean = jnp.mean(normed_grad, axis=-1, keepdims=True)
    second_mean = jnp.mean(normed_grad * normed, axis=-1, keepdims=True)
    return inverse * (normed_grad - first_mean - normed * second_mean)


def times(left_side, right_side):
    return jnp.dot(left_side, right_side, preferred_element_type=jnp.float32)


def inner_rows(left_side, right_side):
    return lax.dot_general(
        left_side, right_side, (((0,), (0,)), ((), ())), preferred_element_type=jnp.float32
    )


def times_transpose(left_side, right_side):
    return lax.dot_general(
        left_side, right_side, (((1,), (1,)), ((), ())), preferred_element_type=jnp.float32
    )


def round_up(value, unit):
    return -(-value // unit) * unit


def chip_grid(chips):
    fast = max(f for f in range(1, chips + 1) if chips % f == 0 and f * f * f <= chips)
    rest = chips // fast
    middle = max(f for f in range(1, rest + 1) if rest % f == 0 and f * f <= rest)
    return (rest // middle, middle, fast)


def chip_ring(chips):
    slow, middle, fast = chip_grid(chips)
    columns = []
    for m in range(middle):
        row = range(fast) if m % 2 == 0 else range(fast - 1, -1, -1)
        columns += [(m, f) for f in row]
    order = []
    for at, (m, f) in enumerate(columns):
        along = range(slow) if at % 2 == 0 else range(slow - 1, -1, -1)
        order += [(s * middle + m) * fast + f for s in along]
    return order


def split_rows_kernel(features, parts, joint_ref, output_ref, wide_ref, out_ref, scratch):
    rows = out_ref.shape[0]
    tiles = joint_ref.shape[1] // LANES
    tail = features - (tiles - 1) * LANES
    keep = lax.broadcasted_iota(jnp.int32, (rows, LANES), 1) < tail
    for t in range(tiles):
        columns = slice(t * LANES, (t + 1) * LANES)
        scratch[t] = joint_ref[:, columns].astype(jnp.float32)
        out = output_ref[:, columns].astype(jnp.float32)
        if t == tiles - 1:
            out = jnp.where(keep, out, 0.0)
        out_ref[:, columns] = out.astype(jnp.bfloat16)
        for p in range(parts):
            piece = scratch[t, pl.ds(p, rows, stride=parts), :]
            if t == tiles - 1:
                piece = jnp.where(keep, piece, 0.0)
            wide_ref[:, (p * tiles + t) * LANES : (p * tiles + t + 1) * LANES] = piece.astype(
                jnp.bfloat16
            )


def split_rows(attention_rows, features, parts=3):
    width = attention_rows.shape[1]
    rows = 64
    steps = features // rows
    return pl.pallas_call(
        functools.partial(split_rows_kernel, features, parts),
        out_shape=(
            jax.ShapeDtypeStruct((features, parts * width), jnp.bfloat16),
            jax.ShapeDtypeStruct((features, width), jnp.bfloat16),
        ),
        grid=(steps,),
        in_specs=[
            pl.BlockSpec((parts * rows, width), lambda i: (i, 0)),
            pl.BlockSpec((rows, width), lambda i: (parts * steps + i, 0)),
        ],
        out_specs=(
            pl.BlockSpec((rows, parts * width), lambda i: (i, 0)),
            pl.BlockSpec((rows, width), lambda i: (i, 0)),
        ),
        scratch_shapes=[pltpu.VMEM((width // LANES, parts * rows, LANES), jnp.float32)],
    )(attention_rows, attention_rows)


def merge_rows_kernel(parts, wide_ref, joint_ref, scratch):
    rows = wide_ref.shape[0]
    tiles = joint_ref.shape[1] // LANES
    for t in range(tiles):
        for p in range(parts):
            scratch[t, pl.ds(p, rows, stride=parts), :] = wide_ref[
                :, (p * tiles + t) * LANES : (p * tiles + t + 1) * LANES
            ].astype(jnp.float32)
        joint_ref[:, t * LANES : (t + 1) * LANES] = scratch[t].astype(jnp.bfloat16)


def merge_rows(wide, parts=3):
    features, width = wide.shape[0], wide.shape[1] // parts
    rows = 64
    return pl.pallas_call(
        functools.partial(merge_rows_kernel, parts),
        out_shape=jax.ShapeDtypeStruct((parts * features, width), jnp.bfloat16),
        grid=(features // rows,),
        in_specs=[pl.BlockSpec((rows, parts * width), lambda i: (i, 0))],
        out_specs=pl.BlockSpec((parts * rows, width), lambda i: (i, 0)),
        scratch_shapes=[pltpu.VMEM((width // LANES, parts * rows, LANES), jnp.float32)],
    )(wide)


def flip(matrix):
    return matrix.astype(jnp.float32).T


def attention_forward_kernel(block, bias_ref, q_ref, k_ref, v_ref, o_ref, lse_ref):
    total = q_ref.shape[0]
    low = lax.broadcasted_iota(jnp.int32, (total, LANES), 1) < HEAD_DIM
    keys = k_ref[...]
    zero = jnp.zeros_like(keys)
    key_parts = (jnp.where(low, keys, zero), jnp.where(low, zero, keys))
    values_t = flip(v_ref[...]).astype(jnp.bfloat16)
    lse_ref[...] = jnp.zeros_like(lse_ref)
    for at in range(total // block):
        span = slice(at * block, (at + 1) * block)
        many = (at + 1) * block
        queries = q_ref[span, :]
        mixed = []
        for h in range(2):
            scores = HEAD_DIM ** (-0.5) * times_transpose(key_parts[h][:many], queries)
            scores = scores + bias_ref[:many, span]
            highest = jnp.max(scores, axis=0, keepdims=True)
            powers = jnp.exp(scores - highest)
            total_power = jnp.sum(powers, axis=0, keepdims=True)
            lse_ref[h : h + 1, span] = highest + jnp.log(total_power)
            probs = (powers * (1.0 / total_power)).astype(jnp.bfloat16)
            mixed.append(times(values_t[h * HEAD_DIM : (h + 1) * HEAD_DIM, :many], probs))
        o_ref[span, :] = jnp.concatenate(mixed, axis=0).T.astype(jnp.bfloat16)


def attention_forward(joint, bias, block=256):
    total = joint.shape[0]
    pairs = joint.shape[1] // (3 * LANES)
    return pl.pallas_call(
        functools.partial(attention_forward_kernel, block),
        out_shape=(
            jax.ShapeDtypeStruct((total, pairs * LANES), jnp.bfloat16),
            jax.ShapeDtypeStruct((pairs * 8, total), jnp.float32),
        ),
        grid=(pairs,),
        in_specs=[
            pl.BlockSpec((total, total), lambda p: (0, 0)),
            pl.BlockSpec((total, LANES), lambda p: (0, p)),
            pl.BlockSpec((total, LANES), lambda p: (0, pairs + p)),
            pl.BlockSpec((total, LANES), lambda p: (0, 2 * pairs + p)),
        ],
        out_specs=(
            pl.BlockSpec((total, LANES), lambda p: (0, p)),
            pl.BlockSpec((8, total), lambda p: (p, 0)),
        ),
    )(bias, joint, joint, joint)


def attention_backward_kernel(
    block, bias_ref, q_ref, k_ref, v_ref, o_ref, g_ref, lse_ref,
    dq_ref, dk_ref, dv_ref, sums_ref, key_sum, value_sum,
):
    total = q_ref.shape[0]
    scale = HEAD_DIM ** (-0.5)
    low = lax.broadcasted_iota(jnp.int32, (total, LANES), 1) < HEAD_DIM
    low_block = low[:block]
    keys, values = k_ref[...], v_ref[...]
    zero = jnp.zeros_like(keys)
    key_parts = (jnp.where(low, keys, zero), jnp.where(low, zero, keys))
    value_parts = (jnp.where(low, values, zero), jnp.where(low, zero, values))
    keys_t = flip(keys).astype(jnp.bfloat16)
    product = flip(g_ref[...]) * flip(o_ref[...])
    deltas = [
        jnp.sum(product[h * HEAD_DIM : (h + 1) * HEAD_DIM], axis=0, keepdims=True) for h in range(2)
    ]
    key_sum[...] = jnp.zeros_like(key_sum)
    value_sum[...] = jnp.zeros_like(value_sum)
    query_columns = jnp.zeros((1, LANES), jnp.float32)
    for at in range(total // block):
        span = slice(at * block, (at + 1) * block)
        many = (at + 1) * block
        queries, grads = q_ref[span, :], g_ref[span, :]
        none = jnp.zeros_like(queries)
        query_parts = (
            jnp.where(low_block, queries, none),
            jnp.where(low_block, none, queries),
        )
        grad_parts = (jnp.where(low_block, grads, none), jnp.where(low_block, none, grads))
        query_grads = []
        key_more, value_more = None, None
        for h in range(2):
            scores = scale * times_transpose(key_parts[h][:many], queries) + bias_ref[:many, span]
            weights = jnp.exp(scores - lse_ref[h : h + 1, span])
            probs = weights.astype(jnp.bfloat16)
            prob_grad = times_transpose(value_parts[h][:many], grads)
            score_grad = (scale * weights * (prob_grad - deltas[h][:, span])).astype(jnp.bfloat16)
            query_grads.append(
                times(keys_t[h * HEAD_DIM : (h + 1) * HEAD_DIM, :many], score_grad)
            )
            key_term = times(score_grad, query_parts[h])
            value_term = times(probs, grad_parts[h])
            key_more = key_term if h == 0 else key_more + key_term
            value_more = value_term if h == 0 else value_more + value_term
        key_sum[:many, :] += key_more
        value_sum[:many, :] += value_more
        query_grad = jnp.concatenate(query_grads, axis=0).T
        query_columns += jnp.sum(query_grad, axis=0, keepdims=True)
        dq_ref[span, :] = query_grad.astype(jnp.bfloat16)
    dk_ref[...] = key_sum[...].astype(jnp.bfloat16)
    dv_ref[...] = value_sum[...].astype(jnp.bfloat16)
    sums_ref[...] = jnp.zeros_like(sums_ref)
    sums_ref[0:1, :] = query_columns
    sums_ref[1:2, :] = jnp.sum(value_sum[...], axis=0, keepdims=True)


def attention_backward(joint, bias, mixed, mixed_grad, lse, block=256):
    total = joint.shape[0]
    pairs = joint.shape[1] // (3 * LANES)
    column = pl.BlockSpec((total, LANES), lambda p: (0, p))
    grad = jax.ShapeDtypeStruct((total, pairs * LANES), jnp.bfloat16)
    return pl.pallas_call(
        functools.partial(attention_backward_kernel, block),
        out_shape=(grad, grad, grad, jax.ShapeDtypeStruct((8, pairs * LANES), jnp.float32)),
        grid=(pairs,),
        in_specs=[
            pl.BlockSpec((total, total), lambda p: (0, 0)),
            column,
            pl.BlockSpec((total, LANES), lambda p: (0, pairs + p)),
            pl.BlockSpec((total, LANES), lambda p: (0, 2 * pairs + p)),
            column,
            column,
            pl.BlockSpec((8, total), lambda p: (p, 0)),
        ],
        out_specs=(column, column, column, pl.BlockSpec((8, LANES), lambda p: (0, p))),
        scratch_shapes=[pltpu.VMEM((total, LANES), jnp.float32)] * 2,
    )(bias, joint, joint, joint, mixed, mixed_grad, lse)


def local(axis, count, tokens, cotangent, segments, attention_flat, feedforward_flat, vectors):
    row_count, features = tokens.shape
    width = round_up(features, LANES)
    spare = width - features
    chips = count // 2
    half_chips = chips // 2
    device = lax.axis_index(axis)
    core, chip = device % 2, device // 2
    partner = [(i, i ^ 1) for i in range(count)]
    ring = chip_ring(chips)
    place = [ring.index(k) for k in range(chips)]
    rings = [[2 * k + c for k in ring] for c in range(2)]

    def swap(value):
        return lax.ppermute(value, axis, partner)

    def by_core(own, other):
        return jnp.where(core == 0, own, other), jnp.where(core == 0, other, own)

    def wide(matrix, to):
        return jnp.pad(matrix, ((0, 0), (0, to - matrix.shape[1])))

    attention_part = attention_flat.reshape(-1, features)
    feed_part = feedforward_flat.reshape(-1, features)
    part_rows, feed_rows = attention_part.shape[0], feed_part.shape[0]
    hidden = feed_rows * count // 2
    hidden_half = hidden // 2
    hidden_block = hidden // chips
    blocks = half_chips
    vector_count = vectors.shape[0]
    vector_rows = -(-vector_count // spare)
    vector_block = jnp.pad(vectors, (0, part_rows * spare - vector_count)).reshape(part_rows, spare)
    attention_rows = lax.all_gather(
        jnp.concatenate([attention_part, vector_block], axis=1), axis, axis=0, tiled=True
    )

    expand_rows = feed_rows * features // hidden
    expand_part = feed_part.reshape(expand_rows, blocks, 2, hidden_block)
    expand_own = lax.dynamic_index_in_dim(expand_part, core, 2, False).reshape(expand_rows, -1)
    expand_send = lax.dynamic_index_in_dim(expand_part, 1 - core, 2, False).reshape(expand_rows, -1)
    expand_pay = wide(
        jnp.concatenate(by_core(expand_own, swap(expand_send)), axis=0), 2 * width
    )
    pay_rows = expand_pay.shape[0]
    contract_pay = wide(feed_part, width).reshape(2, pay_rows, width)
    contract_pay = jnp.concatenate([contract_pay[0], contract_pay[1]], axis=1)
    feed_pay = jnp.where(chip < half_chips, expand_pay, contract_pay)
    feed_all = lax.all_gather(feed_pay, axis, axis=0, axis_index_groups=rings)
    expand_weight = jnp.concatenate([feed_all[place[k]] for k in range(half_chips)], axis=0)
    expand_weight = expand_weight[:, :hidden_half]
    contract_weight = jnp.stack([feed_all[place[half_chips + k]] for k in range(half_chips)])
    contract_weight = (
        contract_weight.reshape(half_chips, pay_rows, 2, width)
        .transpose(0, 2, 1, 3)
        .reshape(hidden_half, width)[:, :features]
    )

    joint_weight, output_weight = split_rows(attention_rows, features)
    vector_all = attention_rows.reshape(count, part_rows, width)[:, :vector_rows, features:]
    vector_all = vector_all.reshape(count, -1)[:, :vector_count].reshape(-1).astype(jnp.float32)
    gains = vector_all[: 8 * features].reshape(8, features)
    expand_bias = vector_all[8 * features :].reshape(blocks, 2, hidden_block)
    expand_bias = lax.dynamic_index_in_dim(expand_bias, core, 1, False).reshape(-1)

    live_rows = (segments >= 0)[:, None]
    positions = jnp.arange(row_count, dtype=jnp.int32)
    visible = (segments[:, None] == segments[None, :]) & (positions[:, None] <= positions[None, :])
    bias = jnp.where(visible, 0.0, masked_score)
    upstream = jnp.where(live_rows, cotangent.astype(jnp.float32), 0.0)
    upstream_low = upstream.astype(jnp.bfloat16)
    upstream_two = jnp.concatenate([upstream_low, swap(upstream_low)], axis=0)

    inputs = tokens.astype(jnp.float32)
    normed_one, inverse_one = normalize(inputs)
    attention_input = (normed_one * gains[0] + gains[1]).astype(jnp.bfloat16)
    edge = jnp.zeros((spare,), jnp.float32)
    joint_bias = jnp.concatenate([gains[2], edge, jnp.zeros((width,), jnp.float32), gains[3], edge])
    joint = (times(attention_input, joint_weight) + joint_bias).astype(jnp.bfloat16)
    mixed, lse = attention_forward(joint, bias)
    mixed_rows = mixed[:, :features]
    output_weight = output_weight[:, :features]
    residual = inputs + times(mixed_rows, output_weight) + gains[4]
    normed_two, inverse_two = normalize(residual)
    feed_input = (normed_two * gains[5] + gains[6]).astype(jnp.bfloat16)

    feed_two = jnp.concatenate([feed_input, swap(feed_input)], axis=0)
    pre_activation = times(feed_two, expand_weight) + expand_bias
    activation = gaussian_unit(pre_activation).astype(jnp.bfloat16)
    activation_grad = times_transpose(upstream_two, contract_weight)
    pre_grad = jax.vjp(gaussian_unit, pre_activation)[1](activation_grad)[0]
    pre_grad_low = pre_grad.astype(jnp.bfloat16)
    expand_bias_grad = jnp.sum(pre_grad, axis=0)
    contract_grad = inner_rows(activation, upstream_two).astype(jnp.bfloat16)
    expand_grad = inner_rows(feed_two, pre_grad_low).astype(jnp.bfloat16)
    expand_pieces = wide(expand_grad, 2 * width).reshape(half_chips, pay_rows, 2 * width)
    contract_pieces = wide(contract_grad, width).reshape(half_chips, 2, pay_rows, width)
    contract_pieces = jnp.concatenate([contract_pieces[:, 0], contract_pieces[:, 1]], axis=2)
    feed_grads = jnp.stack(
        [
            expand_pieces[k] if k < half_chips else contract_pieces[k - half_chips]
            for k in ring
        ]
    )
    feed_sum = lax.psum_scatter(
        feed_grads, axis, scatter_dimension=0, tiled=True, axis_index_groups=rings
    ).reshape(pay_rows, 2 * width)

    second_two = times_transpose(pre_grad_low, expand_weight)
    second_grad = second_two[:row_count] + swap(second_two[row_count:])
    final_two = times(activation, contract_weight)
    final_rows = residual + (final_two[:row_count] + swap(final_two[row_count:])) + gains[7]
    layer_output = jnp.where(live_rows, final_rows, 0.0).astype(jnp.bfloat16)

    contract_bias_grad = jnp.sum(upstream, axis=0)
    second_gain_grad = jnp.sum(second_grad * normed_two, axis=0)
    second_bias_grad = jnp.sum(second_grad, axis=0)
    residual_grad = upstream + normalize_back(second_grad * gains[5], normed_two, inverse_two)
    residual_low = residual_grad.astype(jnp.bfloat16)
    output_grad = inner_rows(mixed_rows, residual_low).astype(jnp.bfloat16)
    output_bias_grad = jnp.sum(residual_grad, axis=0)
    mixed_grad = wide(times_transpose(residual_low, output_weight).astype(jnp.bfloat16), width)
    query_grad, key_grad, value_grad, column_sums = attention_backward(
        joint, bias, mixed, mixed_grad, lse
    )
    joint_low = jnp.concatenate([query_grad, key_grad, value_grad], axis=1)
    joint_grad = merge_rows(inner_rows(attention_input, joint_low).astype(jnp.bfloat16))
    first_grad = times_transpose(joint_low, joint_weight)
    first_gain_grad = jnp.sum(first_grad * normed_one, axis=0)
    first_bias_grad = jnp.sum(first_grad, axis=0)
    token_gradient = residual_grad + normalize_back(
        first_grad * gains[0], normed_one, inverse_one
    )

    expand_bias_all = jnp.zeros((blocks, 2, hidden_block), jnp.float32)
    expand_bias_all = lax.dynamic_update_slice(
        expand_bias_all, expand_bias_grad.reshape(blocks, 1, hidden_block), (0, core, 0)
    )
    vector_grad = jnp.concatenate(
        [
            first_gain_grad,
            first_bias_grad,
            column_sums[0, :features],
            column_sums[1, :features],
            output_bias_grad,
            second_gain_grad,
            second_bias_grad,
            contract_bias_grad,
            expand_bias_all.reshape(-1),
        ]
    ).astype(jnp.bfloat16)
    vector_grad = jnp.pad(
        vector_grad.reshape(count, vector_count), ((0, 0), (0, vector_rows * spare - vector_count))
    ).reshape(count, vector_rows, spare)
    attention_grads = jnp.concatenate([joint_grad, wide(output_grad, width)], axis=0)
    attention_grads = attention_grads.reshape(count, part_rows, width)
    attention_grads = attention_grads.at[:, :vector_rows, features:].set(vector_grad)
    attention_grads = attention_grads.reshape(chips, 2, part_rows, width)
    away = lax.dynamic_index_in_dim(attention_grads, 1 - core, 1, False)
    stay = lax.dynamic_index_in_dim(attention_grads, core, 1, False)
    chip_grads = (stay.astype(jnp.float32) + swap(away).astype(jnp.float32)).astype(jnp.bfloat16)
    chip_grads = jnp.stack([chip_grads[k] for k in ring])
    attention_sum = lax.psum_scatter(
        chip_grads, axis, scatter_dimension=0, tiled=True, axis_index_groups=rings
    ).reshape(part_rows, width)
    attention_gradient = attention_sum[:, :features].astype(jnp.float32).reshape(-1, LANES)
    vector_gradient = attention_sum[:vector_rows, features:].reshape(-1)[:vector_count]
    vector_gradient = vector_gradient.astype(jnp.float32)

    rows_zero, rows_one = feed_sum[:expand_rows], feed_sum[expand_rows:]
    rows_own, rows_away = by_core(rows_zero, rows_one)
    part_zero, part_one = by_core(rows_own, swap(rows_away))
    expand_sum = jnp.stack(
        [
            part_zero[:, :hidden_half].reshape(expand_rows, blocks, hidden_block),
            part_one[:, :hidden_half].reshape(expand_rows, blocks, hidden_block),
        ],
        axis=2,
    ).reshape(feed_rows, features)
    contract_sum = jnp.concatenate(
        [feed_sum[:, :features], feed_sum[:, width : width + features]], axis=0
    )
    feed_sum = jnp.where(chip < half_chips, expand_sum, contract_sum)
    feedforward_gradient = feed_sum.astype(jnp.float32).reshape(-1, LANES)
    return (layer_output, token_gradient, attention_gradient, feedforward_gradient, vector_gradient)


def solution(mesh):
    axis = mesh.axis_names[0]
    in_specs = (P(axis, None), P(axis, None), P(axis), P(axis, None), P(axis, None), P(axis))
    out_specs = (P(axis, None), P(axis, None), P(axis, None), P(axis, None), P(axis))
    return jax.shard_map(
        functools.partial(local, axis, mesh.shape[axis]),
        mesh=mesh,
        in_specs=in_specs,
        out_specs=out_specs,
        check_vma=False,
    )
```

```python
import functools

import jax
import jax.numpy as jnp
from jax import lax
from jax.experimental import pallas as pl
from jax.experimental.pallas import tpu as pltpu
from jax.sharding import PartitionSpec as P

HEAD_DIM = 64
LANES = 128

norm_epsilon = 1e-05
masked_score = -1e30


def gaussian_unit(values):
    return jax.nn.gelu(values, approximate=True)


def normalize(matrix):
    center = jnp.mean(matrix, axis=-1, keepdims=True)
    deviation = matrix - center
    variance = jnp.mean(deviation * deviation, axis=-1, keepdims=True)
    inverse = lax.rsqrt(variance + norm_epsilon)
    return (deviation * inverse, inverse)


def normalize_back(normed_grad, normed, inverse):
    first_mean = jnp.mean(normed_grad, axis=-1, keepdims=True)
    second_mean = jnp.mean(normed_grad * normed, axis=-1, keepdims=True)
    return inverse * (normed_grad - first_mean - normed * second_mean)


def times(left_side, right_side):
    return jnp.dot(left_side, right_side, preferred_element_type=jnp.float32)


def inner_rows(left_side, right_side):
    return lax.dot_general(
        left_side, right_side, (((0,), (0,)), ((), ())), preferred_element_type=jnp.float32
    )


def times_transpose(left_side, right_side):
    return lax.dot_general(
        left_side, right_side, (((1,), (1,)), ((), ())), preferred_element_type=jnp.float32
    )


def round_up(value, unit):
    return -(-value // unit) * unit


def chip_grid(chips):
    fast = max(f for f in range(1, chips + 1) if chips % f == 0 and f * f * f <= chips)
    rest = chips // fast
    middle = max(f for f in range(1, rest + 1) if rest % f == 0 and f * f <= rest)
    return (rest // middle, middle, fast)


def chip_ring(chips):
    slow, middle, fast = chip_grid(chips)
    columns = []
    for m in range(middle):
        row = range(fast) if m % 2 == 0 else range(fast - 1, -1, -1)
        columns += [(m, f) for f in row]
    order = []
    for at, (m, f) in enumerate(columns):
        along = range(slow) if at % 2 == 0 else range(slow - 1, -1, -1)
        order += [(s * middle + m) * fast + f for s in along]
    return order


def split_rows_kernel(features, parts, joint_ref, output_ref, wide_ref, out_ref, scratch):
    rows = out_ref.shape[0]
    tiles = joint_ref.shape[1] // LANES
    tail = features - (tiles - 1) * LANES
    keep = lax.broadcasted_iota(jnp.int32, (rows, LANES), 1) < tail
    for t in range(tiles):
        columns = slice(t * LANES, (t + 1) * LANES)
        scratch[t] = joint_ref[:, columns].astype(jnp.float32)
        out = output_ref[:, columns].astype(jnp.float32)
        if t == tiles - 1:
            out = jnp.where(keep, out, 0.0)
        out_ref[:, columns] = out.astype(jnp.bfloat16)
        for p in range(parts):
            piece = scratch[t, pl.ds(p, rows, stride=parts), :]
            if t == tiles - 1:
                piece = jnp.where(keep, piece, 0.0)
            wide_ref[:, (p * tiles + t) * LANES : (p * tiles + t + 1) * LANES] = piece.astype(
                jnp.bfloat16
            )


def split_rows(attention_rows, features, parts=3):
    width = attention_rows.shape[1]
    rows = 64
    steps = features // rows
    return pl.pallas_call(
        functools.partial(split_rows_kernel, features, parts),
        out_shape=(
            jax.ShapeDtypeStruct((features, parts * width), jnp.bfloat16),
            jax.ShapeDtypeStruct((features, width), jnp.bfloat16),
        ),
        grid=(steps,),
        in_specs=[
            pl.BlockSpec((parts * rows, width), lambda i: (i, 0)),
            pl.BlockSpec((rows, width), lambda i: (parts * steps + i, 0)),
        ],
        out_specs=(
            pl.BlockSpec((rows, parts * width), lambda i: (i, 0)),
            pl.BlockSpec((rows, width), lambda i: (i, 0)),
        ),
        scratch_shapes=[pltpu.VMEM((width // LANES, parts * rows, LANES), jnp.float32)],
    )(attention_rows, attention_rows)


def merge_rows_kernel(parts, wide_ref, joint_ref, scratch):
    rows = wide_ref.shape[0]
    tiles = joint_ref.shape[1] // LANES
    for t in range(tiles):
        for p in range(parts):
            scratch[t, pl.ds(p, rows, stride=parts), :] = wide_ref[
                :, (p * tiles + t) * LANES : (p * tiles + t + 1) * LANES
            ].astype(jnp.float32)
        joint_ref[:, t * LANES : (t + 1) * LANES] = scratch[t].astype(jnp.bfloat16)


def merge_rows(wide, parts=3):
    features, width = wide.shape[0], wide.shape[1] // parts
    rows = 64
    return pl.pallas_call(
        functools.partial(merge_rows_kernel, parts),
        out_shape=jax.ShapeDtypeStruct((parts * features, width), jnp.bfloat16),
        grid=(features // rows,),
        in_specs=[pl.BlockSpec((rows, parts * width), lambda i: (i, 0))],
        out_specs=pl.BlockSpec((parts * rows, width), lambda i: (i, 0)),
        scratch_shapes=[pltpu.VMEM((width // LANES, parts * rows, LANES), jnp.float32)],
    )(wide)


def flip(matrix):
    return matrix.astype(jnp.float32).T


def attention_forward_kernel(block, bias_ref, q_ref, k_ref, v_ref, o_ref, lse_ref):
    total = q_ref.shape[0]
    low = lax.broadcasted_iota(jnp.int32, (total, LANES), 1) < HEAD_DIM
    keys = k_ref[...]
    zero = jnp.zeros_like(keys)
    key_parts = (jnp.where(low, keys, zero), jnp.where(low, zero, keys))
    values_t = flip(v_ref[...]).astype(jnp.bfloat16)
    lse_ref[...] = jnp.zeros_like(lse_ref)
    for at in range(total // block):
        span = slice(at * block, (at + 1) * block)
        many = (at + 1) * block
        queries = q_ref[span, :]
        mixed = []
        for h in range(2):
            scores = HEAD_DIM ** (-0.5) * times_transpose(key_parts[h][:many], queries)
            scores = scores + bias_ref[:many, span]
            highest = jnp.max(scores, axis=0, keepdims=True)
            powers = jnp.exp(scores - highest)
            total_power = jnp.sum(powers, axis=0, keepdims=True)
            lse_ref[h : h + 1, span] = highest + jnp.log(total_power)
            probs = (powers * (1.0 / total_power)).astype(jnp.bfloat16)
            mixed.append(times(values_t[h * HEAD_DIM : (h + 1) * HEAD_DIM, :many], probs))
        o_ref[span, :] = jnp.concatenate(mixed, axis=0).T.astype(jnp.bfloat16)


def attention_forward(joint, bias, block=256):
    total = joint.shape[0]
    pairs = joint.shape[1] // (3 * LANES)
    return pl.pallas_call(
        functools.partial(attention_forward_kernel, block),
        out_shape=(
            jax.ShapeDtypeStruct((total, pairs * LANES), jnp.bfloat16),
            jax.ShapeDtypeStruct((pairs * 8, total), jnp.float32),
        ),
        grid=(pairs,),
        in_specs=[
            pl.BlockSpec((total, total), lambda p: (0, 0)),
            pl.BlockSpec((total, LANES), lambda p: (0, p)),
            pl.BlockSpec((total, LANES), lambda p: (0, pairs + p)),
            pl.BlockSpec((total, LANES), lambda p: (0, 2 * pairs + p)),
        ],
        out_specs=(
            pl.BlockSpec((total, LANES), lambda p: (0, p)),
            pl.BlockSpec((8, total), lambda p: (p, 0)),
        ),
    )(bias, joint, joint, joint)


def attention_backward_kernel(
    block, bias_ref, q_ref, k_ref, v_ref, o_ref, g_ref, lse_ref,
    dq_ref, dk_ref, dv_ref, sums_ref, key_sum, value_sum,
):
    total = q_ref.shape[0]
    scale = HEAD_DIM ** (-0.5)
    low = lax.broadcasted_iota(jnp.int32, (total, LANES), 1) < HEAD_DIM
    low_block = low[:block]
    keys, values = k_ref[...], v_ref[...]
    zero = jnp.zeros_like(keys)
    key_parts = (jnp.where(low, keys, zero), jnp.where(low, zero, keys))
    value_parts = (jnp.where(low, values, zero), jnp.where(low, zero, values))
    keys_t = flip(keys).astype(jnp.bfloat16)
    product = flip(g_ref[...]) * flip(o_ref[...])
    deltas = [
        jnp.sum(product[h * HEAD_DIM : (h + 1) * HEAD_DIM], axis=0, keepdims=True) for h in range(2)
    ]
    key_sum[...] = jnp.zeros_like(key_sum)
    value_sum[...] = jnp.zeros_like(value_sum)
    query_columns = jnp.zeros((1, LANES), jnp.float32)
    for at in range(total // block):
        span = slice(at * block, (at + 1) * block)
        many = (at + 1) * block
        queries, grads = q_ref[span, :], g_ref[span, :]
        none = jnp.zeros_like(queries)
        query_parts = (
            jnp.where(low_block, queries, none),
            jnp.where(low_block, none, queries),
        )
        grad_parts = (jnp.where(low_block, grads, none), jnp.where(low_block, none, grads))
        query_grads = []
        key_more, value_more = None, None
        for h in range(2):
            scores = scale * times_transpose(key_parts[h][:many], queries) + bias_ref[:many, span]
            weights = jnp.exp(scores - lse_ref[h : h + 1, span])
            probs = weights.astype(jnp.bfloat16)
            prob_grad = times_transpose(value_parts[h][:many], grads)
            score_grad = (scale * weights * (prob_grad - deltas[h][:, span])).astype(jnp.bfloat16)
            query_grads.append(
                times(keys_t[h * HEAD_DIM : (h + 1) * HEAD_DIM, :many], score_grad)
            )
            key_term = times(score_grad, query_parts[h])
            value_term = times(probs, grad_parts[h])
            key_more = key_term if h == 0 else key_more + key_term
            value_more = value_term if h == 0 else value_more + value_term
        key_sum[:many, :] += key_more
        value_sum[:many, :] += value_more
        query_grad = jnp.concatenate(query_grads, axis=0).T
        query_columns += jnp.sum(query_grad, axis=0, keepdims=True)
        dq_ref[span, :] = query_grad.astype(jnp.bfloat16)
    dk_ref[...] = key_sum[...].astype(jnp.bfloat16)
    dv_ref[...] = value_sum[...].astype(jnp.bfloat16)
    sums_ref[...] = jnp.zeros_like(sums_ref)
    sums_ref[0:1, :] = query_columns
    sums_ref[1:2, :] = jnp.sum(value_sum[...], axis=0, keepdims=True)


def attention_backward(joint, bias, mixed, mixed_grad, lse, block=256):
    total = joint.shape[0]
    pairs = joint.shape[1] // (3 * LANES)
    column = pl.BlockSpec((total, LANES), lambda p: (0, p))
    grad = jax.ShapeDtypeStruct((total, pairs * LANES), jnp.bfloat16)
    return pl.pallas_call(
        functools.partial(attention_backward_kernel, block),
        out_shape=(grad, grad, grad, jax.ShapeDtypeStruct((8, pairs * LANES), jnp.float32)),
        grid=(pairs,),
        in_specs=[
            pl.BlockSpec((total, total), lambda p: (0, 0)),
            column,
            pl.BlockSpec((total, LANES), lambda p: (0, pairs + p)),
            pl.BlockSpec((total, LANES), lambda p: (0, 2 * pairs + p)),
            column,
            column,
            pl.BlockSpec((8, total), lambda p: (p, 0)),
        ],
        out_specs=(column, column, column, pl.BlockSpec((8, LANES), lambda p: (0, p))),
        scratch_shapes=[pltpu.VMEM((total, LANES), jnp.float32)] * 2,
    )(bias, joint, joint, joint, mixed, mixed_grad, lse)


def gather_kernel(axis, grid, part_ref, out_ref, own_sem, z_sems, x_sems, y_sems, c_sems):
    nz, ny, nx = grid
    rows = part_ref.shape[0]
    me = lax.axis_index(axis)
    c = me % 2
    x = me // 2 % nx
    y = me // (2 * nx) % ny
    z = me // (2 * nx * ny)

    def at(z, y, x, c):
        return ((z * ny + y) * nx + x) * 2 + c

    half = min(-(-rows // 16) * 8, rows)
    halves = (pl.ds(0, half), pl.ds(half, rows - half))

    barrier = pltpu.get_barrier_semaphore()
    count = 1
    pl.semaphore_signal(barrier, inc=1, device_id=at(z, y, x, 1 - c), device_id_type=pl.DeviceIdType.LOGICAL)
    for size, spot, to in ((nz, z, lambda v: at(v, y, x, c)), (ny, y, lambda v: at(z, v, x, c)), (nx, x, lambda v: at(z, y, v, c))):
        for step in (-1, 1):
            there = (spot + step >= 0) & (spot + step < size)

            @pl.when(there)
            def _(to=to, spot=spot, step=step):
                pl.semaphore_signal(barrier, inc=1, device_id=to(spot + step), device_id_type=pl.DeviceIdType.LOGICAL)

            count = count + there.astype(jnp.int32)
    pl.semaphore_wait(barrier, count)

    own = pltpu.make_async_copy(part_ref, out_ref.at[z, y, x, c], own_sem)
    own.start()

    def copy(src, dst, sems, index, device):
        return pltpu.make_async_remote_copy(
            src_ref=src, dst_ref=dst, send_sem=sems.at[(0, *index)], recv_sem=sems.at[(1, *index)],
            device_id=device, device_id_type=pl.DeviceIdType.LOGICAL,
        )

    def z_copy(s, way):
        source = z - way * (s - 1)
        ok = (source >= 0) & (source < nz) & (z + way >= 0) & (z + way < nz)
        ref = out_ref.at[jnp.clip(source, 0, nz - 1), y, x, c]
        src = part_ref if s == 1 else ref
        return ok, copy(src, ref, z_sems, (s - 1, (way + 1) // 2), at(jnp.clip(z + way, 0, nz - 1), y, x, c))

    def z_came(s, way):
        source = z - way * s
        ok = (source >= 0) & (source < nz)
        ref = out_ref.at[jnp.clip(source, 0, nz - 1), y, x, c]
        return ok, copy(ref, ref, z_sems, (s - 1, (way + 1) // 2), me)

    def line(color, second, zz, s, way):
        along_x = (color == 0) != second
        size, spot = (nx, x) if along_x else (ny, y)
        sems = x_sems if along_x else y_sems
        index = (zz, int(second), s - 1, (way + 1) // 2)

        def block(v):
            v = jnp.clip(v, 0, size - 1)
            if second:
                where = (zz, slice(None), v) if along_x else (zz, v, slice(None))
            else:
                where = (zz, y, v) if along_x else (zz, v, x)
            return out_ref.at[(*where, c, halves[color])]

        target = jnp.clip(spot + way, 0, size - 1)
        target = at(z, y, target, c) if along_x else at(z, target, x, c)
        source = spot - way * (s - 1)
        ok = (source >= 0) & (source < size) & (spot + way >= 0) & (spot + way < size)
        send = copy(block(source), block(source), sems, index, target)
        came = spot - way * s
        came_ok = (came >= 0) & (came < size)
        recv = copy(block(came), block(came), sems, index, me)
        return ok, send, came_ok, recv

    def line_sends(color, second, zz, s):
        for way in (-1, 1):
            ok, send, _, _ = line(color, second, zz, s, way)

            @pl.when(ok)
            def _(send=send):
                send.start()

    def line_waits(color, second, zz, s):
        for way in (-1, 1):
            _, _, ok, recv = line(color, second, zz, s, way)

            @pl.when(ok)
            def _(recv=recv):
                recv.wait_recv()

    def length(color, second):
        return (nx if (color == 0) != second else ny) - 1

    def core_copy(zz, device):
        ref = out_ref.at[zz, :, :, c]
        return copy(ref, ref, c_sems, (zz,), device)

    def each(columns, act):
        for o in columns:
            zz = z + o

            @pl.when((zz >= 0) & (zz < nz))
            def _(zz=zz):
                act(jnp.clip(zz, 0, nz - 1))

    def first(zz):
        for color in (0, 1):
            if length(color, False) > 0:
                line_sends(color, False, zz, 1)

    def middle(zz):
        most = max(length(0, False), length(1, False))
        for s in range(1, most + 1):
            for color in (0, 1):
                if s <= length(color, False):
                    line_waits(color, False, zz, s)
                    if s < length(color, False):
                        line_sends(color, False, zz, s + 1)
                    elif length(color, True) > 0:
                        line_sends(color, True, zz, 1)

    def last(zz):
        most = max(length(0, True), length(1, True))
        for s in range(1, most + 1):
            for color in (0, 1):
                if s <= length(color, True):
                    line_waits(color, True, zz, s)
                    if s < length(color, True):
                        line_sends(color, True, zz, s + 1)
        core_copy(zz, at(z, y, x, 1 - c)).start()

    def came(s):
        return (0,) if s == 0 else (-s, s)

    for way in (-1, 1):
        if nz > 1:
            ok, send = z_copy(1, way)

            @pl.when(ok)
            def _(send=send):
                send.start()
    own.wait()
    each(came(0), first)
    for s in range(1, nz):
        for way in (-1, 1):
            ok, recv = z_came(s, way)

            @pl.when(ok)
            def _(recv=recv):
                recv.wait_recv()

            if s < nz - 1:
                ok, send = z_copy(s + 1, way)

                @pl.when(ok)
                def _(send=send):
                    send.start()
        each(came(s - 1), middle)
        each(came(s), first)
        if s > 1:
            each(came(s - 2), last)
    each(came(nz - 1), middle)
    if nz > 1:
        each(came(nz - 2), last)
    each(came(nz - 1), last)

    for s in range(1, nz):
        for way in (-1, 1):
            ok, send = z_copy(s, way)

            @pl.when(ok)
            def _(send=send):
                send.wait_send()
    for zz in range(nz):
        for second in (False, True):
            for color in (0, 1):
                for s in range(1, length(color, second) + 1):
                    for way in (-1, 1):
                        ok, send, _, _ = line(color, second, zz, s, way)

                        @pl.when(ok)
                        def _(send=send):
                            send.wait_send()
        core_copy(zz, at(z, y, x, 1 - c)).wait_send()
        ref = out_ref.at[zz, :, :, 1 - c]
        copy(ref, ref, c_sems, (zz,), me).wait_recv()


def gather_rows(part, axis, count, collective_id):
    grid = chip_grid(count // 2)
    nz, ny, nx = grid
    out = pl.pallas_call(
        functools.partial(gather_kernel, axis, grid),
        out_shape=jax.ShapeDtypeStruct((*grid, 2, *part.shape), part.dtype),
        in_specs=[pl.BlockSpec(memory_space=pltpu.VMEM)],
        out_specs=pl.BlockSpec(memory_space=pl.ANY),
        scratch_shapes=[
            pltpu.SemaphoreType.DMA,
            pltpu.SemaphoreType.DMA((2, max(nz - 1, 1), 2)),
            pltpu.SemaphoreType.DMA((2, nz, 2, max(nx - 1, 1), 2)),
            pltpu.SemaphoreType.DMA((2, nz, 2, max(ny - 1, 1), 2)),
            pltpu.SemaphoreType.DMA((2, nz)),
        ],
        compiler_params=pltpu.CompilerParams(collective_id=collective_id, has_side_effects=True),
    )(part)
    return out.reshape(count, *part.shape)


def local(axis, count, tokens, cotangent, segments, attention_flat, feedforward_flat, vectors):
    row_count, features = tokens.shape
    width = round_up(features, LANES)
    spare = width - features
    chips = count // 2
    half_chips = chips // 2
    device = lax.axis_index(axis)
    core, chip = device % 2, device // 2
    partner = [(i, i ^ 1) for i in range(count)]
    ring = chip_ring(chips)
    place = [ring.index(k) for k in range(chips)]
    rings = [[2 * k + c for k in ring] for c in range(2)]

    def swap(value):
        return lax.ppermute(value, axis, partner)

    def by_core(own, other):
        return jnp.where(core == 0, own, other), jnp.where(core == 0, other, own)

    def wide(matrix, to):
        return jnp.pad(matrix, ((0, 0), (0, to - matrix.shape[1])))

    attention_part = attention_flat.reshape(-1, features)
    feed_part = feedforward_flat.reshape(-1, features)
    part_rows, feed_rows = attention_part.shape[0], feed_part.shape[0]
    hidden = feed_rows * count // 2
    hidden_half = hidden // 2
    hidden_block = hidden // chips
    blocks = half_chips
    vector_count = vectors.shape[0]
    vector_rows = -(-vector_count // spare)
    vector_block = jnp.pad(vectors, (0, part_rows * spare - vector_count)).reshape(part_rows, spare)
    attention_rows = gather_rows(
        jnp.concatenate([attention_part, vector_block], axis=1), axis, count, 1
    ).reshape(-1, width)

    expand_rows = feed_rows * features // hidden
    expand_part = feed_part.reshape(expand_rows, blocks, 2, hidden_block)
    expand_own = lax.dynamic_index_in_dim(expand_part, core, 2, False).reshape(expand_rows, -1)
    expand_send = lax.dynamic_index_in_dim(expand_part, 1 - core, 2, False).reshape(expand_rows, -1)
    expand_pay = wide(
        jnp.concatenate(by_core(expand_own, swap(expand_send)), axis=0), 2 * width
    )
    pay_rows = expand_pay.shape[0]
    contract_pay = wide(feed_part, width).reshape(2, pay_rows, width)
    contract_pay = jnp.concatenate([contract_pay[0], contract_pay[1]], axis=1)
    feed_pay = jnp.where(chip < half_chips, expand_pay, contract_pay)
    feed_all = lax.all_gather(feed_pay, axis, axis=0, axis_index_groups=rings)
    expand_weight = jnp.concatenate([feed_all[place[k]] for k in range(half_chips)], axis=0)
    expand_weight = expand_weight[:, :hidden_half]
    contract_weight = jnp.stack([feed_all[place[half_chips + k]] for k in range(half_chips)])
    contract_weight = (
        contract_weight.reshape(half_chips, pay_rows, 2, width)
        .transpose(0, 2, 1, 3)
        .reshape(hidden_half, width)[:, :features]
    )

    joint_weight, output_weight = split_rows(attention_rows, features)
    vector_all = attention_rows.reshape(count, part_rows, width)[:, :vector_rows, features:]
    vector_all = vector_all.reshape(count, -1)[:, :vector_count].reshape(-1).astype(jnp.float32)
    gains = vector_all[: 8 * features].reshape(8, features)
    expand_bias = vector_all[8 * features :].reshape(blocks, 2, hidden_block)
    expand_bias = lax.dynamic_index_in_dim(expand_bias, core, 1, False).reshape(-1)

    live_rows = (segments >= 0)[:, None]
    positions = jnp.arange(row_count, dtype=jnp.int32)
    visible = (segments[:, None] == segments[None, :]) & (positions[:, None] <= positions[None, :])
    bias = jnp.where(visible, 0.0, masked_score)
    upstream = jnp.where(live_rows, cotangent.astype(jnp.float32), 0.0)
    upstream_low = upstream.astype(jnp.bfloat16)
    upstream_two = jnp.concatenate([upstream_low, swap(upstream_low)], axis=0)

    inputs = tokens.astype(jnp.float32)
    normed_one, inverse_one = normalize(inputs)
    attention_input = (normed_one * gains[0] + gains[1]).astype(jnp.bfloat16)
    edge = jnp.zeros((spare,), jnp.float32)
    joint_bias = jnp.concatenate([gains[2], edge, jnp.zeros((width,), jnp.float32), gains[3], edge])
    joint = (times(attention_input, joint_weight) + joint_bias).astype(jnp.bfloat16)
    mixed, lse = attention_forward(joint, bias)
    mixed_rows = mixed[:, :features]
    output_weight = output_weight[:, :features]
    residual = inputs + times(mixed_rows, output_weight) + gains[4]
    normed_two, inverse_two = normalize(residual)
    feed_input = (normed_two * gains[5] + gains[6]).astype(jnp.bfloat16)

    feed_two = jnp.concatenate([feed_input, swap(feed_input)], axis=0)
    pre_activation = times(feed_two, expand_weight) + expand_bias
    activation = gaussian_unit(pre_activation).astype(jnp.bfloat16)
    activation_grad = times_transpose(upstream_two, contract_weight)
    pre_grad = jax.vjp(gaussian_unit, pre_activation)[1](activation_grad)[0]
    pre_grad_low = pre_grad.astype(jnp.bfloat16)
    expand_bias_grad = jnp.sum(pre_grad, axis=0)
    contract_grad = inner_rows(activation, upstream_two).astype(jnp.bfloat16)
    expand_grad = inner_rows(feed_two, pre_grad_low).astype(jnp.bfloat16)
    expand_pieces = wide(expand_grad, 2 * width).reshape(half_chips, pay_rows, 2 * width)
    contract_pieces = wide(contract_grad, width).reshape(half_chips, 2, pay_rows, width)
    contract_pieces = jnp.concatenate([contract_pieces[:, 0], contract_pieces[:, 1]], axis=2)
    feed_grads = jnp.stack(
        [
            expand_pieces[k] if k < half_chips else contract_pieces[k - half_chips]
            for k in ring
        ]
    )
    feed_grads, pre_grad_low, activation = lax.optimization_barrier(
        (feed_grads, pre_grad_low, activation)
    )
    feed_sum = lax.psum_scatter(
        feed_grads, axis, scatter_dimension=0, tiled=True, axis_index_groups=rings
    ).reshape(pay_rows, 2 * width)

    second_two = times_transpose(pre_grad_low, expand_weight)
    second_grad = second_two[:row_count] + swap(second_two[row_count:])
    final_two = times(activation, contract_weight)
    final_rows = residual + (final_two[:row_count] + swap(final_two[row_count:])) + gains[7]
    layer_output = jnp.where(live_rows, final_rows, 0.0).astype(jnp.bfloat16)

    contract_bias_grad = jnp.sum(upstream, axis=0)
    second_gain_grad = jnp.sum(second_grad * normed_two, axis=0)
    second_bias_grad = jnp.sum(second_grad, axis=0)
    residual_grad = upstream + normalize_back(second_grad * gains[5], normed_two, inverse_two)
    residual_low = residual_grad.astype(jnp.bfloat16)
    output_grad = inner_rows(mixed_rows, residual_low).astype(jnp.bfloat16)
    output_bias_grad = jnp.sum(residual_grad, axis=0)
    mixed_grad = wide(times_transpose(residual_low, output_weight).astype(jnp.bfloat16), width)
    query_grad, key_grad, value_grad, column_sums = attention_backward(
        joint, bias, mixed, mixed_grad, lse
    )
    joint_low = jnp.concatenate([query_grad, key_grad, value_grad], axis=1)
    joint_grad = merge_rows(inner_rows(attention_input, joint_low).astype(jnp.bfloat16))
    first_grad = times_transpose(joint_low, joint_weight)
    first_gain_grad = jnp.sum(first_grad * normed_one, axis=0)
    first_bias_grad = jnp.sum(first_grad, axis=0)
    token_gradient = residual_grad + normalize_back(
        first_grad * gains[0], normed_one, inverse_one
    )

    expand_bias_all = jnp.zeros((blocks, 2, hidden_block), jnp.float32)
    expand_bias_all = lax.dynamic_update_slice(
        expand_bias_all, expand_bias_grad.reshape(blocks, 1, hidden_block), (0, core, 0)
    )
    vector_grad = jnp.concatenate(
        [
            first_gain_grad,
            first_bias_grad,
            column_sums[0, :features],
            column_sums[1, :features],
            output_bias_grad,
            second_gain_grad,
            second_bias_grad,
            contract_bias_grad,
            expand_bias_all.reshape(-1),
        ]
    ).astype(jnp.bfloat16)
    vector_grad = jnp.pad(
        vector_grad.reshape(count, vector_count), ((0, 0), (0, vector_rows * spare - vector_count))
    ).reshape(count, vector_rows, spare)
    attention_grads = jnp.concatenate([joint_grad, wide(output_grad, width)], axis=0)
    attention_grads = attention_grads.reshape(count, part_rows, width)
    attention_grads = attention_grads.at[:, :vector_rows, features:].set(vector_grad)
    attention_grads = attention_grads.reshape(chips, 2, part_rows, width)
    away = lax.dynamic_index_in_dim(attention_grads, 1 - core, 1, False)
    stay = lax.dynamic_index_in_dim(attention_grads, core, 1, False)
    chip_grads = (stay.astype(jnp.float32) + swap(away).astype(jnp.float32)).astype(jnp.bfloat16)
    chip_grads = jnp.stack([chip_grads[k] for k in ring])
    attention_sum = lax.psum_scatter(
        chip_grads, axis, scatter_dimension=0, tiled=True, axis_index_groups=rings
    ).reshape(part_rows, width)
    attention_gradient = attention_sum[:, :features].astype(jnp.float32).reshape(-1, LANES)
    vector_gradient = attention_sum[:vector_rows, features:].reshape(-1)[:vector_count]
    vector_gradient = vector_gradient.astype(jnp.float32)

    rows_zero, rows_one = feed_sum[:expand_rows], feed_sum[expand_rows:]
    rows_own, rows_away = by_core(rows_zero, rows_one)
    part_zero, part_one = by_core(rows_own, swap(rows_away))
    expand_sum = jnp.stack(
        [
            part_zero[:, :hidden_half].reshape(expand_rows, blocks, hidden_block),
            part_one[:, :hidden_half].reshape(expand_rows, blocks, hidden_block),
        ],
        axis=2,
    ).reshape(feed_rows, features)
    contract_sum = jnp.concatenate(
        [feed_sum[:, :features], feed_sum[:, width : width + features]], axis=0
    )
    feed_sum = jnp.where(chip < half_chips, expand_sum, contract_sum)
    feedforward_gradient = feed_sum.astype(jnp.float32).reshape(-1, LANES)
    return (layer_output, token_gradient, attention_gradient, feedforward_gradient, vector_gradient)


def solution(mesh):
    axis = mesh.axis_names[0]
    in_specs = (P(axis, None), P(axis, None), P(axis), P(axis, None), P(axis, None), P(axis))
    out_specs = (P(axis, None), P(axis, None), P(axis, None), P(axis, None), P(axis))
    return jax.shard_map(
        functools.partial(local, axis, mesh.shape[axis]),
        mesh=mesh,
        in_specs=in_specs,
        out_specs=out_specs,
        check_vma=False,
    )
```
